32 devices in a mesh: dom: 8 (over z, x), sub: 4 (over y, core).
Axes of the slice: x: 2, y: 2, z: 4, core: 2. Of those that a mesh axis runs over, the one named last changes fastest.
Arguments:
- level_set: float32 [64, 32, 128], P('dom', 'sub'), may hold values from 0 to 1
- velocity: float32 [3, 64, 32, 128], P(None, 'dom', 'sub'), may hold values from -6 to 6
- source: float32 [64, 32, 128], P('dom', 'sub'), may hold values from -12 to 12
Outputs:
- new_level: float32 [64, 32, 128], P('dom', 'sub')
- pressure: float32 [64, 32, 128], P('dom', 'sub')
- correction: float32 [64, 32, 128], P('dom', 'sub')
The draws below stay inside these ranges and needn't reach their ends.
All inputs are finite; a program needn't handle non-finite values.
Results may differ from the reference program's by a relative error of at most 0.0003.
Values sent between devices are 32-bit elements; how exact they have to be, the bound alone decides.
A program may use at most 64 MiB of HBM per device.

```python
import math
import jax
import jax.numpy as jnp
import numpy as np
from jax import lax

SWEEPS = 2
PITERS = 2
NX = 64
NY = 32
NZ = 128


def draw_level_set(key, part):
    spread_key = jax.random.fold_in(key, 11)
    noise_key = jax.random.fold_in(key, 12)
    log_scale = jax.random.uniform(spread_key, (NX // 8, NY // 8, NZ // 8), jnp.float32, math.log(0.005), math.log(0.5))
    amplitude = jnp.exp(log_scale)
    amplitude = jnp.repeat(jnp.repeat(jnp.repeat(amplitude, 8, axis=0), 8, axis=1), 8, axis=2)
    across = jnp.arange(NX, dtype=jnp.float32)[:, None, None] / NX
    along = jnp.arange(NY, dtype=jnp.float32)[None, :, None] / NY
    smooth_base = 0.5 + 0.25 * jnp.sin(2.0 * math.pi * across) * jnp.cos(2.0 * math.pi * along)
    rough_part = jnp.clip(0.2 * jax.random.normal(noise_key, (NX, NY, NZ), jnp.float32), -0.5, 0.5)
    return smooth_base + amplitude * rough_part


def draw_source(key, part):
    share_dom = jnp.arange(NX, dtype=jnp.float32)[:, None, None] / NX
    share_sub = jnp.arange(NY, dtype=jnp.float32)[None, :, None] / NY
    spread = 1.0 + share_dom + share_sub
    random_part = jnp.clip(jax.random.normal(key, (NX, NY, NZ), jnp.float32), -4.0, 4.0)
    return random_part * spread


def shard_levels(key, dims, split, low, high):
    gain, own = 1.0, jax.random.fold_in(key, 6)
    for position, shards_of in split:
        draws = jnp.exp(jax.random.uniform(jax.random.fold_in(own, position), (shards_of,), jnp.float32, low / len(split), high / len(split)))
        gain = gain * jnp.repeat(draws, dims[position] // shards_of).reshape([-1 if axis == position else 1 for axis in range(len(dims))])
    return gain


def bell_draw(stream_key, extent, scale, most, cuts=(), held_as=jnp.bfloat16):
    entries = jax.random.normal(stream_key, extent, jnp.float32) * scale
    if len(cuts) > 0:
        entries = shard_levels(stream_key, extent, cuts, -0.22, 0.18) * entries
    return jnp.clip(entries, min=-most, max=most).astype(held_as)


def setup_inputs(seed: int = 0) -> dict:
    arg_keys = jax.random.split(jax.random.key(seed), 4)
    return {
        "level_set": draw_level_set(jax.random.fold_in(arg_keys[3], 71), 0),
        "velocity": bell_draw(arg_keys[1], (3, NX, NY, NZ), 1.0, 6.0, ((1, 8), (2, 4)), jnp.float32),
        "source": draw_source(jax.random.fold_in(arg_keys[3], 71), 0),
    }


gll_nodes = [-1.0, -0.8717401485096066, -0.5917001814331423, -0.2092992179024789, 0.2092992179024789, 0.5917001814331423, 0.8717401485096066, 1.0]
advect_step = 0.05
reinit_step = 0.02
interface_width = 0.1
density_ratio = 9.0

def tables():
    node_points = np.array(gll_nodes)
    poly_order = 7
    values_prev = np.ones(8)
    values_now = node_points.copy()
    for degree in range(1, poly_order):
        values_next = ((2 * degree + 1) * node_points * values_now - degree * values_prev) / (degree + 1)
        values_prev, values_now = (values_now, values_next)
    matrix = np.zeros((8, 8))
    for line in range(8):
        for column in range(8):
            if line != column:
                matrix[line, column] = values_now[line] / (values_now[column] * (node_points[line] - node_points[column]))
    matrix[0, 0] = -poly_order * (poly_order + 1) / 4.0
    matrix[7, 7] = poly_order * (poly_order + 1) / 4.0
    weights = 2.0 / (poly_order * (poly_order + 1) * values_now ** 2)
    return (matrix, weights)

def point_tables(full_shape, weights):
    corner_count = np.array([2.0, 1.0, 1.0, 1.0, 1.0, 1.0, 1.0, 2.0])
    weight_lines = []
    count_lines = []
    for dim_index in (1, 2, 3):
        repeats = full_shape[dim_index] // 8
        weight_lines.append(jnp.asarray(np.tile(weights, repeats), jnp.float32))
        count_lines.append(jnp.asarray(np.tile(1.0 / corner_count, repeats), jnp.float32))
    weight_cube = (weight_lines[0][:, None, None] * weight_lines[1][None, :, None] * weight_lines[2][None, None, :])[None]
    inv_mult = (count_lines[0][:, None, None] * count_lines[1][None, :, None] * count_lines[2][None, None, :])[None]
    return (weight_cube, inv_mult)

def derive(values, dim_index, matrix):
    full_shape = values.shape
    highest = lax.Precision.HIGHEST
    table = jnp.asarray(matrix, jnp.float32)
    if dim_index == 1:
        blocks = values.reshape((full_shape[0], full_shape[1] // 8, 8) + full_shape[2:])
        result = jnp.einsum('baipq,ji->bajpq', blocks, table, precision=highest)
    elif dim_index == 2:
        blocks = values.reshape(full_shape[:2] + (full_shape[2] // 8, 8, full_shape[3]))
        result = jnp.einsum('bpaiq,ji->bpajq', blocks, table, precision=highest)
    else:
        blocks = values.reshape(full_shape[:3] + (full_shape[3] // 8, 8))
        result = jnp.einsum('bpqai,ji->bpqaj', blocks, table, precision=highest)
    return result.reshape(full_shape)

def gradient(values, matrix):
    return [derive(values, 1, matrix), derive(values, 2, matrix), derive(values, 3, matrix)]

def fold_faces(padded, dim_index, length):
    inner_part = lax.slice_in_dim(padded, 1, length + 1, axis=dim_index)
    left_face = lax.slice_in_dim(inner_part, 0, length, 8, dim_index) + lax.slice_in_dim(padded, 0, length, 8, dim_index)
    right_face = lax.slice_in_dim(inner_part, 7, length, 8, dim_index) + lax.slice_in_dim(padded, 9, length + 2, 8, dim_index)
    full_shape = inner_part.shape
    split_shape = full_shape[:dim_index] + (length // 8, 8) + full_shape[dim_index + 1:]
    middle = lax.slice_in_dim(inner_part.reshape(split_shape), 1, 7, axis=dim_index + 1)
    joined = jnp.concatenate([jnp.expand_dims(left_face, dim_index + 1), middle, jnp.expand_dims(right_face, dim_index + 1)], axis=dim_index + 1)
    return joined.reshape(full_shape)

def wrap_pad(values, dim_index):
    length = values.shape[dim_index]
    return jnp.concatenate([lax.slice_in_dim(values, length - 1, length, axis=dim_index), values, lax.slice_in_dim(values, 0, 1, axis=dim_index)], axis=dim_index)

def assemble(values):
    for dim_index in (1, 2, 3):
        values = fold_faces(wrap_pad(values, dim_index), dim_index, values.shape[dim_index])
    return values

def reference(level_set, velocity, source):
    matrix, weights = tables()
    phase_field = level_set[None]
    weight_cube, inv_mult = point_tables(phase_field.shape, weights)
    gradients = gradient(phase_field, matrix)
    advected = phase_field - advect_step * (velocity[0:1] * gradients[0] + velocity[1:2] * gradients[1] + velocity[2:3] * gradients[2])
    phase_field = assemble(advected) * inv_mult
    gradients = gradient(phase_field, matrix)
    magnitude = jnp.sqrt(gradients[0] * gradients[0] + gradients[1] * gradients[1] + gradients[2] * gradients[2])
    scaled = 1.0 / jnp.maximum(magnitude, 1.0)
    normals = [gradients[0] * scaled, gradients[1] * scaled, gradients[2] * scaled]
    for sweep_index in range(SWEEPS):
        if sweep_index > 0:
            gradients = gradient(phase_field, matrix)
        compress = phase_field * (1.0 - phase_field)
        change = derive(interface_width * gradients[0] - compress * normals[0], 1, matrix)
        change = change + derive(interface_width * gradients[1] - compress * normals[1], 2, matrix)
        change = change + derive(interface_width * gradients[2] - compress * normals[2], 3, matrix)
        phase_field = phase_field + reinit_step * assemble(change) * inv_mult
    mobility = 1.0 / (1.0 + density_ratio * phase_field * phase_field)
    weighted = weight_cube * mobility
    square_t = (matrix * matrix).T
    diag_local = weight_cube + derive(weighted, 1, square_t) + derive(weighted, 2, square_t) + derive(weighted, 3, square_t)
    assembled = assemble(jnp.concatenate([weight_cube * source[None], diag_local], axis=0))
    right_side = assembled[0:1]
    diagonal = assembled[1:2]
    transposed = matrix.T

    def operate(direction):
        grads_dir = gradient(direction, matrix)
        local_sum = weight_cube * direction + derive(weighted * grads_dir[0], 1, transposed)
        local_sum = local_sum + derive(weighted * grads_dir[1], 2, transposed) + derive(weighted * grads_dir[2], 3, transposed)
        return assemble(local_sum)

    def inner_product(first_vec, second_vec):
        return jnp.sum(first_vec * second_vec * inv_mult)
    solution = jnp.zeros_like(right_side)
    residual = right_side
    precond = residual / diagonal
    direction = precond
    norm_now = inner_product(residual, precond)
    for step_index in range(PITERS):
        applied = operate(direction)
        step_size = norm_now / inner_product(direction, applied)
        solution = solution + step_size * direction
        residual = residual - step_size * applied
        if step_index + 1 < PITERS:
            precond = residual / diagonal
            norm_next = inner_product(residual, precond)
            direction = precond + norm_next / norm_now * direction
            norm_now = norm_next
    return (phase_field[0], solution[0], (residual / diagonal)[0])
```

```python
import functools

import jax
import jax.numpy as jnp
import numpy as np
from jax import lax
from jax.experimental import pallas as pl
from jax.experimental.pallas import tpu as pltpu
from jax.sharding import PartitionSpec as P

SWEEPS = 2
PITERS = 2
MESH = pl.DeviceIdType.MESH


gll_nodes = [
    -1.0,
    -0.8717401485096066,
    -0.5917001814331423,
    -0.2092992179024789,
    0.2092992179024789,
    0.5917001814331423,
    0.8717401485096066,
    1.0,
]
advect_step = 0.05
reinit_step = 0.02
interface_width = 0.1
density_ratio = 9.0
ORDER = 8
GRAD, TRANS, SQUARE = 0, 1, 2


def tables():
    node_points = np.array(gll_nodes)
    poly_order = 7
    values_prev = np.ones(8)
    values_now = node_points.copy()
    for degree in range(1, poly_order):
        values_next = ((2 * degree + 1) * node_points * values_now - degree * values_prev) / (
            degree + 1
        )
        values_prev, values_now = (values_now, values_next)
    matrix = np.zeros((8, 8))
    for line in range(8):
        for column in range(8):
            if line != column:
                matrix[line, column] = values_now[line] / (
                    values_now[column] * (node_points[line] - node_points[column])
                )
    matrix[0, 0] = -poly_order * (poly_order + 1) / 4.0
    matrix[7, 7] = poly_order * (poly_order + 1) / 4.0
    weights = 2.0 / (poly_order * (poly_order + 1) * values_now**2)
    return (matrix, weights)


MATRIX, WEIGHTS = tables()
KINDS = (MATRIX, MATRIX.T, (MATRIX * MATRIX).T)
COUNT = np.array([0.5, 1.0, 1.0, 1.0, 1.0, 1.0, 1.0, 0.5])


def constants(lanes):
    rows = np.arange(ORDER)
    planes = []
    for matrix in KINDS:
        for shift in range(ORDER):
            column = matrix[rows, (rows - shift) % ORDER]
            planes.append(np.broadcast_to(column[:, None], (ORDER, lanes)))
    repeats = lanes // ORDER
    planes.append(WEIGHTS[:, None] * np.tile(WEIGHTS, repeats)[None, :])
    planes.append(COUNT[:, None] * np.tile(COUNT, repeats)[None, :])
    planes = np.stack(planes).astype(np.float32)
    wide = []
    for matrix in KINDS:
        full = np.kron(np.eye(repeats), matrix.T).astype(np.float32)
        high = full.astype(jnp.bfloat16)
        low = (full - high.astype(np.float32)).astype(jnp.bfloat16)
        wide.append(np.concatenate([high, low], axis=1))
    return planes, np.stack(wide)


def along_first(values, kind):
    matrix = KINDS[kind]
    half = ORDER // 2
    flip = -1.0 if kind != SQUARE else 1.0
    even = [values[i] + values[ORDER - 1 - i] for i in range(half)]
    odd = [values[i] - values[ORDER - 1 - i] for i in range(half)]
    front, back = [], []
    for j in range(half):
        even_sum = odd_sum = None
        for i in range(half):
            ce = float(0.5 * (matrix[j, i] + matrix[j, ORDER - 1 - i]))
            co = float(0.5 * (matrix[j, i] - matrix[j, ORDER - 1 - i]))
            even_sum = even[i] * ce if even_sum is None else even_sum + even[i] * ce
            odd_sum = odd[i] * co if odd_sum is None else odd_sum + odd[i] * co
        front.append(even_sum + odd_sum)
        back.append(flip * (even_sum - odd_sum))
    return front + back[::-1]


def kernel(ndom, nsub, local_barrier, level_ref, velocity_ref, source_ref, planes_ref, wide_ref,
           new_ref, pressure_ref, correction_ref, *scratch):
    (level_v, velocity_v, source_v, planes_v, wide_v, out_v, in_sem, out_sem,
     face_send, face_recv, edge_send, edge_recv, sum_send, sum_recv,
     first_faces, first_edges, first_faces_in, first_edges_in,
     faces, edges, faces_in, edges_in, sums, sums_in) = scratch
    dom, sub = lax.axis_index("dom"), lax.axis_index("sub")

    def peer(a, b):
        return (lax.rem(dom + a % ndom, ndom), lax.rem(sub + b % nsub, nsub))

    loads = [
        pltpu.make_async_copy(src, dst, in_sem.at[i])
        for i, (src, dst) in enumerate((
            (level_ref, level_v), (planes_ref, planes_v), (wide_ref, wide_v),
            (velocity_ref, velocity_v), (source_ref, source_v)))
    ]
    barrier = pltpu.get_barrier_semaphore()
    near = [(a, b) for a in (-1, 1, 0) for b in (-1, 1, 0) if a or b]
    if local_barrier:
        for a, b in near:
            pl.semaphore_signal(barrier, inc=1, device_id=peer(a, b), device_id_type=MESH)
    else:
        @pl.loop(1, ndom * nsub)
        def _(k):
            target = (lax.rem(dom + k // nsub, ndom), lax.rem(sub + k % nsub, nsub))
            pl.semaphore_signal(barrier, inc=1, device_id=target, device_id_type=MESH)
    for load in loads:
        load.start()

    shape = level_v.shape[1:]
    lane = lax.broadcasted_iota(jnp.int32, shape, 1) % ORDER
    row = lax.broadcasted_iota(jnp.int32, shape, 0)
    lane_first, lane_last = lane == 0, lane == ORDER - 1
    row_first, row_last = row == 0, row == ORDER - 1
    lanes = shape[1]
    span = range(ORDER)

    def fold_lanes(v):
        lower = pltpu.roll(v, 1, 1)
        upper = pltpu.roll(v, lanes - 1, 1)
        return v + jnp.where(lane_last, upper, jnp.where(lane_first, lower, 0.0))

    def along_second(values, kind):
        result = []
        for v in values:
            total = v * planes_v[kind * ORDER]
            for shift in range(1, ORDER):
                total = total + pltpu.roll(v, shift, 0) * planes_v[kind * ORDER + shift]
            result.append(total)
        return result

    def along_third(values, kind):
        stacked = jnp.concatenate(values, axis=0)
        high = stacked.astype(jnp.bfloat16)
        low = (stacked - high.astype(jnp.float32)).astype(jnp.bfloat16)
        out = jnp.dot(jnp.concatenate([high, low], axis=0), wide_v[kind],
                      preferred_element_type=jnp.float32)
        n = ORDER * ORDER
        total = out[:n, :lanes] + (out[:n, lanes:] + out[n:, :lanes])
        return [total[i * ORDER:(i + 1) * ORDER] for i in span]

    def gradient(values):
        third = along_third(values, GRAD)
        return along_first(values, GRAD), along_second(values, GRAD), third

    def divergence(parts, kind):
        third = along_third(parts[2], kind)
        first, second = along_first(parts[0], kind), along_second(parts[1], kind)
        return [(first[i] + second[i]) + third[i] for i in span]

    def send(slot, fields, face_out, edge_out, face_in, edge_in):
        fields = [[fold_lanes(v) for v in field] for field in fields]
        for n, field in enumerate(fields):
            face_out[0, n] = field[ORDER - 1]
            face_out[1, n] = field[0]
            right = jnp.concatenate([v[ORDER - 1:] for v in field], axis=0)
            left = jnp.concatenate([v[:1] for v in field], axis=0)
            face_out[2, n] = right
            face_out[3, n] = left
            edge_out[0, n] = field[ORDER - 1][ORDER - 1:]
            edge_out[1, n] = field[ORDER - 1][:1]
            edge_out[2, n] = field[0][ORDER - 1:]
            edge_out[3, n] = field[0][:1]
        for i, (a, b) in enumerate(((1, 1), (1, -1), (-1, 1), (-1, -1))):
            pltpu.make_async_remote_copy(
                edge_out.at[i], edge_in.at[i], edge_send.at[slot], edge_recv.at[slot],
                device_id=peer(a, b), device_id_type=MESH).start()
        for i, (a, b) in enumerate(((1, 0), (-1, 0), (0, 1), (0, -1))):
            pltpu.make_async_remote_copy(
                face_out.at[i], face_in.at[i], face_send.at[slot], face_recv.at[slot],
                device_id=peer(a, b), device_id_type=MESH).start()
        return fields

    def receive(slot, fields, face_in, edge_in):
        pltpu.make_async_copy(face_in, face_in, face_recv.at[slot]).wait()
        pltpu.make_async_copy(edge_in, edge_in, edge_recv.at[slot]).wait()
        results = []
        for n, field in enumerate(fields):
            result = list(field)
            result[0] = result[0] + face_in[0, n]
            result[ORDER - 1] = result[ORDER - 1] + face_in[1, n]
            for i, (at, mask_a, mask_b) in enumerate((
                    (0, row_first, row_last), (ORDER - 1, row_first, row_last))):
                result[at] = result[at] + jnp.where(
                    mask_a, edge_in[2 * i, n],
                    jnp.where(mask_b, edge_in[2 * i + 1, n], 0.0))
            for i in span:
                result[i] = result[i] + jnp.where(
                    row_first, face_in[2, n, i:i + 1],
                    jnp.where(row_last, face_in[3, n, i:i + 1], 0.0))
            results.append(result)
        return results

    def begin(step, field):
        buffers = (faces.at[step], edges.at[step], faces_in.at[step], edges_in.at[step])
        return send(step + 1, [field], *buffers)

    def finish(step, field):
        return receive(step + 1, field, faces_in.at[step], edges_in.at[step])[0]

    def assemble(step, field):
        return finish(step, begin(step, field))

    hops = sorted(range(ndom), key=lambda a: -min(a, ndom - a))
    others = [(a, b) for a in hops for b in (2, 1, 3, 0) if a or b] if nsub == 4 else [
        (a, b) for a in hops for b in range(nsub) if a or b]

    def begin_sums(step, first, second):
        sums[step, 0:1] = jnp.sum(first, axis=0, keepdims=True)
        sums[step, 1:2] = jnp.sum(second, axis=0, keepdims=True)

        def post(target, k):
            pltpu.make_async_remote_copy(
                sums.at[step], sums_in.at[step, k], sum_send.at[step], sum_recv.at[step],
                device_id=target, device_id_type=MESH).start()
        if ndom * nsub <= 64:
            for k, (a, b) in enumerate(others):
                post(peer(a, b), k)
        else:
            @pl.loop(1, ndom * nsub)
            def _(k):
                post((lax.rem(dom + k // nsub, ndom), lax.rem(sub + k % nsub, nsub)), k - 1)

    def finish_sums(step):
        pltpu.make_async_copy(sums_in.at[step], sums_in.at[step], sum_recv.at[step]).wait()
        total = sums[step] + jnp.sum(sums_in[step], axis=0)
        total = jnp.sum(total, axis=1, keepdims=True)
        return total[0:1], total[1:2]

    def dot(a, b, scale=None):
        total = None
        for i in span:
            term = a[i] * b[i]
            if scale is not None:
                term = term * scale[i]
            total = term if total is None else total + term
        return total

    for load in loads[:3]:
        load.wait()
    weight_plane = planes_v[3 * ORDER]
    count_plane = planes_v[3 * ORDER + 1]
    weight = [weight_plane * float(WEIGHTS[i]) for i in span]
    inv_mult = [count_plane * float(COUNT[i]) for i in span]

    phi = [level_v[i] for i in span]
    g0, g1, g2 = gradient(phi)
    loads[3].wait()
    advected = [
        phi[i] - advect_step * (velocity_v[0, i] * g0[i] + velocity_v[1, i] * g1[i]
                                + velocity_v[2, i] * g2[i]) for i in span]
    loads[4].wait()
    right = [weight[i] * source_v[i] for i in span]
    pl.semaphore_wait(barrier, len(near) if local_barrier else ndom * nsub - 1)
    fields = send(0, [advected, right], first_faces, first_edges, first_faces_in, first_edges_in)
    phi, right = receive(0, fields, first_faces_in, first_edges_in)
    phi = [phi[i] * inv_mult[i] for i in span]

    step = 0
    for sweep in range(SWEEPS):
        g0, g1, g2 = gradient(phi)
        if sweep == 0:
            scaled = [lax.rsqrt(jnp.maximum(
                g0[i] * g0[i] + g1[i] * g1[i] + g2[i] * g2[i], 1.0)) for i in span]
            normals = [[g[i] * scaled[i] for i in span] for g in (g0, g1, g2)]
        compress = [p * (1.0 - p) for p in phi]
        flux = [[interface_width * g[i] - compress[i] * normal[i] for i in span]
                for g, normal in zip((g0, g1, g2), normals)]
        change = assemble(step, divergence(flux, GRAD))
        step += 1
        phi = [phi[i] + reinit_step * change[i] * inv_mult[i] for i in span]

    for i in span:
        out_v[0, i] = phi[i]
    stores = [pltpu.make_async_copy(out_v.at[n], ref, out_sem.at[n])
              for n, ref in enumerate((new_ref, pressure_ref, correction_ref))]
    stores[0].start()
    weighted = [weight[i] * (1.0 / (1.0 + density_ratio * phi[i] * phi[i])) for i in span]
    squares = divergence([weighted] * 3, SQUARE)
    diagonal = assemble(step, [weight[i] + squares[i] for i in span])
    step += 1
    inverse = [1.0 / v for v in diagonal]

    def operate(values):
        parts = [[weighted[i] * g[i] for i in span] for g in gradient(values)]
        total = divergence(parts, TRANS)
        return [weight[i] * values[i] + total[i] for i in span]

    def apply(step, sum_step, residual, precond):
        partial = operate(precond)
        sent = begin(step, partial)
        begin_sums(sum_step, dot(residual, precond, inv_mult), dot(precond, partial))
        applied = finish(step, sent)
        return (applied,) + finish_sums(sum_step)

    residual = right
    precond = [residual[i] * inverse[i] for i in span]
    applied, norm_now, product = apply(step, 0, residual, precond)
    step += 1
    step_size = norm_now / product
    direction, image = precond, applied
    result = None
    for it in range(PITERS):
        moved = [step_size * d for d in direction]
        result = moved if result is None else [result[i] + moved[i] for i in span]
        residual = [residual[i] - step_size * image[i] for i in span]
        if it + 1 < PITERS:
            precond = [residual[i] * inverse[i] for i in span]
            applied, norm_next, product = apply(step, it + 1, residual, precond)
            step += 1
            ratio = norm_next / norm_now
            step_size = norm_next / (product - ratio * norm_next / step_size)
            direction = [precond[i] + ratio * direction[i] for i in span]
            image = [applied[i] + ratio * image[i] for i in span]
            norm_now = norm_next
    for i in span:
        out_v[1, i] = result[i]
        out_v[2, i] = residual[i] * inverse[i]
    stores[1].start()
    stores[2].start()
    pltpu.make_async_copy(first_faces, first_faces, face_send.at[0]).wait()
    pltpu.make_async_copy(first_edges, first_edges, edge_send.at[0]).wait()
    for s in range(step):
        pltpu.make_async_copy(faces.at[s], faces.at[s], face_send.at[s + 1]).wait()
        pltpu.make_async_copy(edges.at[s], edges.at[s], edge_send.at[s + 1]).wait()
    for s in range(PITERS):
        pltpu.make_async_copy(sums_in.at[s], sums_in.at[s], sum_send.at[s]).wait()
    for store in stores:
        store.wait()


def solution(mesh):
    ndom, nsub = mesh.shape["dom"], mesh.shape["sub"]
    rounds = SWEEPS + 1 + PITERS
    local_barrier = max(ndom, nsub) // 2 <= SWEEPS + 3

    def local(level_set, velocity, source):
        assert level_set.shape[:2] == (ORDER, ORDER)
        lanes = level_set.shape[2]
        planes, wide = constants(lanes)
        tile = (ORDER, lanes)
        vmem = functools.partial(pltpu.VMEM, dtype=jnp.float32)
        others = ndom * nsub - 1
        dma = pltpu.SemaphoreType.DMA
        scratch = [
            vmem(level_set.shape), vmem(velocity.shape), vmem(source.shape),
            vmem(planes.shape), pltpu.VMEM(wide.shape, jnp.bfloat16),
            vmem((3,) + level_set.shape), dma((5,)), dma((3,)),
            dma((rounds + 1,)), dma((rounds + 1,)), dma((rounds + 1,)), dma((rounds + 1,)),
            dma((PITERS,)), dma((PITERS,)),
            vmem((4, 2) + tile), vmem((4, 2, 1, lanes)),
            vmem((4, 2) + tile), vmem((4, 2, 1, lanes)),
            vmem((rounds, 4, 1) + tile), vmem((rounds, 4, 1, 1, lanes)),
            vmem((rounds, 4, 1) + tile), vmem((rounds, 4, 1, 1, lanes)),
            vmem((PITERS, 2, lanes)), vmem((PITERS, others, 2, lanes)),
        ]
        any_space = pl.BlockSpec(memory_space=pl.ANY)
        out = jax.ShapeDtypeStruct(level_set.shape, jnp.float32)
        return pl.pallas_call(
            functools.partial(kernel, ndom, nsub, local_barrier),
            out_shape=(out, out, out),
            in_specs=[any_space] * 5,
            out_specs=(any_space,) * 3,
            scratch_shapes=scratch,
            compiler_params=pltpu.CompilerParams(collective_id=0, has_side_effects=True),
        )(level_set, velocity, source, jnp.asarray(planes), jnp.asarray(wide))

    return jax.shard_map(
        local,
        mesh=mesh,
        in_specs=(P("dom", "sub", None), P(None, "dom", "sub", None), P("dom", "sub", None)),
        out_specs=(P("dom", "sub", None), P("dom", "sub", None), P("dom", "sub", None)),
        check_vma=False,
    )
```

```python
import functools

import jax
import jax.numpy as jnp
import numpy as np
from jax import lax
from jax.experimental import pallas as pl
from jax.experimental.pallas import tpu as pltpu
from jax.sharding import PartitionSpec as P

SWEEPS = 2
PITERS = 2
MESH = pl.DeviceIdType.MESH


gll_nodes = [
    -1.0,
    -0.8717401485096066,
    -0.5917001814331423,
    -0.2092992179024789,
    0.2092992179024789,
    0.5917001814331423,
    0.8717401485096066,
    1.0,
]
advect_step = 0.05
reinit_step = 0.02
interface_width = 0.1
density_ratio = 9.0
ORDER = 8
GRAD, TRANS, SQUARE = 0, 1, 2


def tables():
    node_points = np.array(gll_nodes)
    poly_order = 7
    values_prev = np.ones(8)
    values_now = node_points.copy()
    for degree in range(1, poly_order):
        values_next = ((2 * degree + 1) * node_points * values_now - degree * values_prev) / (
            degree + 1
        )
        values_prev, values_now = (values_now, values_next)
    matrix = np.zeros((8, 8))
    for line in range(8):
        for column in range(8):
            if line != column:
                matrix[line, column] = values_now[line] / (
                    values_now[column] * (node_points[line] - node_points[column])
                )
    matrix[0, 0] = -poly_order * (poly_order + 1) / 4.0
    matrix[7, 7] = poly_order * (poly_order + 1) / 4.0
    weights = 2.0 / (poly_order * (poly_order + 1) * values_now**2)
    return (matrix, weights)


MATRIX, WEIGHTS = tables()
KINDS = (MATRIX, MATRIX.T, (MATRIX * MATRIX).T)
COUNT = np.array([0.5, 1.0, 1.0, 1.0, 1.0, 1.0, 1.0, 0.5])


def constants(lanes):
    rows = np.arange(ORDER)
    planes = []
    for matrix in KINDS:
        for shift in range(ORDER):
            column = matrix[rows, (rows - shift) % ORDER]
            planes.append(np.broadcast_to(column[:, None], (ORDER, lanes)))
    repeats = lanes // ORDER
    planes.append(WEIGHTS[:, None] * np.tile(WEIGHTS, repeats)[None, :])
    planes.append(COUNT[:, None] * np.tile(COUNT, repeats)[None, :])
    planes = np.stack(planes).astype(np.float32)
    wide = []
    for matrix in KINDS:
        full = np.kron(np.eye(repeats), matrix.T).astype(np.float32)
        high = full.astype(jnp.bfloat16)
        low = (full - high.astype(np.float32)).astype(jnp.bfloat16)
        wide.append(np.concatenate([high, low], axis=1))
    return planes, np.stack(wide)


def along_first(values, kind):
    matrix = KINDS[kind]
    half = ORDER // 2
    flip = -1.0 if kind != SQUARE else 1.0
    even = [values[i] + values[ORDER - 1 - i] for i in range(half)]
    odd = [values[i] - values[ORDER - 1 - i] for i in range(half)]
    front, back = [], []
    for j in range(half):
        even_sum = odd_sum = None
        for i in range(half):
            ce = float(0.5 * (matrix[j, i] + matrix[j, ORDER - 1 - i]))
            co = float(0.5 * (matrix[j, i] - matrix[j, ORDER - 1 - i]))
            even_sum = even[i] * ce if even_sum is None else even_sum + even[i] * ce
            odd_sum = odd[i] * co if odd_sum is None else odd_sum + odd[i] * co
        front.append(even_sum + odd_sum)
        back.append(flip * (even_sum - odd_sum))
    return front + back[::-1]


def kernel(ndom, nsub, local_barrier, level_ref, velocity_ref, source_ref, planes_ref, wide_ref,
           new_ref, pressure_ref, correction_ref, *scratch):
    (level_v, velocity_v, source_v, planes_v, wide_v, in_sem,
     face_send, face_recv, edge_send, edge_recv, sum_send, sum_recv,
     first_faces, first_edges, first_faces_in, first_edges_in,
     faces, edges, faces_in, edges_in, sums, sums_in) = scratch
    dom, sub = lax.axis_index("dom"), lax.axis_index("sub")

    def peer(a, b):
        return (lax.rem(dom + a % ndom, ndom), lax.rem(sub + b % nsub, nsub))

    loads = [
        pltpu.make_async_copy(src, dst, in_sem.at[i])
        for i, (src, dst) in enumerate((
            (level_ref, level_v), (planes_ref, planes_v), (wide_ref, wide_v),
            (velocity_ref, velocity_v), (source_ref, source_v)))
    ]
    barrier = pltpu.get_barrier_semaphore()
    near = [(a, b) for a in (-1, 1, 0) for b in (-1, 1, 0) if a or b]
    if local_barrier:
        for a, b in near:
            pl.semaphore_signal(barrier, inc=1, device_id=peer(a, b), device_id_type=MESH)
    else:
        @pl.loop(1, ndom * nsub)
        def _(k):
            target = (lax.rem(dom + k // nsub, ndom), lax.rem(sub + k % nsub, nsub))
            pl.semaphore_signal(barrier, inc=1, device_id=target, device_id_type=MESH)
    for load in loads:
        load.start()

    shape = level_v.shape[1:]
    lane = lax.broadcasted_iota(jnp.int32, shape, 1) % ORDER
    row = lax.broadcasted_iota(jnp.int32, shape, 0)
    lane_first, lane_last = lane == 0, lane == ORDER - 1
    row_first, row_last = row == 0, row == ORDER - 1
    lanes = shape[1]
    span = range(ORDER)

    def fold_lanes(v):
        lower = pltpu.roll(v, 1, 1)
        upper = pltpu.roll(v, lanes - 1, 1)
        return v + jnp.where(lane_last, upper, jnp.where(lane_first, lower, 0.0))

    def along_second(values, kind):
        result = []
        for v in values:
            total = v * planes_v[kind * ORDER]
            for shift in range(1, ORDER):
                total = total + pltpu.roll(v, shift, 0) * planes_v[kind * ORDER + shift]
            result.append(total)
        return result

    def along_third(values, kind):
        stacked = jnp.concatenate(values, axis=0)
        high = stacked.astype(jnp.bfloat16)
        low = (stacked - high.astype(jnp.float32)).astype(jnp.bfloat16)
        out = jnp.dot(jnp.concatenate([high, low], axis=0), wide_v[kind],
                      preferred_element_type=jnp.float32)
        n = ORDER * ORDER
        total = out[:n, :lanes] + (out[:n, lanes:] + out[n:, :lanes])
        return [total[i * ORDER:(i + 1) * ORDER] for i in span]

    def gradient(values):
        third = along_third(values, GRAD)
        return along_first(values, GRAD), along_second(values, GRAD), third

    def divergence(parts, kind):
        third = along_third(parts[2], kind)
        first, second = along_first(parts[0], kind), along_second(parts[1], kind)
        return [(first[i] + second[i]) + third[i] for i in span]

    def send(slot, fields, face_out, edge_out, face_in, edge_in):
        fields = [[fold_lanes(v) for v in field] for field in fields]
        for n, field in enumerate(fields):
            face_out[0, n] = field[ORDER - 1]
            face_out[1, n] = field[0]
            right = jnp.concatenate([v[ORDER - 1:] for v in field], axis=0)
            left = jnp.concatenate([v[:1] for v in field], axis=0)
            face_out[2, n] = right
            face_out[3, n] = left
            edge_out[0, n] = field[ORDER - 1][ORDER - 1:]
            edge_out[1, n] = field[ORDER - 1][:1]
            edge_out[2, n] = field[0][ORDER - 1:]
            edge_out[3, n] = field[0][:1]
        for i, (a, b) in enumerate(((1, 1), (1, -1), (-1, 1), (-1, -1))):
            pltpu.make_async_remote_copy(
                edge_out.at[i], edge_in.at[i], edge_send.at[slot], edge_recv.at[slot],
                device_id=peer(a, b), device_id_type=MESH).start()
        for i, (a, b) in enumerate(((1, 0), (-1, 0), (0, 1), (0, -1))):
            pltpu.make_async_remote_copy(
                face_out.at[i], face_in.at[i], face_send.at[slot], face_recv.at[slot],
                device_id=peer(a, b), device_id_type=MESH).start()
        return fields

    def receive(slot, fields, face_in, edge_in):
        pltpu.make_async_copy(face_in, face_in, face_recv.at[slot]).wait()
        pltpu.make_async_copy(edge_in, edge_in, edge_recv.at[slot]).wait()
        results = []
        for n, field in enumerate(fields):
            result = list(field)
            result[0] = result[0] + face_in[0, n]
            result[ORDER - 1] = result[ORDER - 1] + face_in[1, n]
            for i, (at, mask_a, mask_b) in enumerate((
                    (0, row_first, row_last), (ORDER - 1, row_first, row_last))):
                result[at] = result[at] + jnp.where(
                    mask_a, edge_in[2 * i, n],
                    jnp.where(mask_b, edge_in[2 * i + 1, n], 0.0))
            for i in span:
                result[i] = result[i] + jnp.where(
                    row_first, face_in[2, n, i:i + 1],
                    jnp.where(row_last, face_in[3, n, i:i + 1], 0.0))
            results.append(result)
        return results

    def begin(step, field):
        buffers = (faces.at[step], edges.at[step], faces_in.at[step], edges_in.at[step])
        return send(step + 1, [field], *buffers)

    def finish(step, field):
        return receive(step + 1, field, faces_in.at[step], edges_in.at[step])[0]

    def assemble(step, field):
        return finish(step, begin(step, field))

    hops = sorted(range(ndom), key=lambda a: -min(a, ndom - a))
    others = [(a, b) for a in hops for b in (2, 1, 3, 0) if a or b] if nsub == 4 else [
        (a, b) for a in hops for b in range(nsub) if a or b]

    def begin_sums(step, first, second):
        sums[step, 0:1] = jnp.sum(first, axis=0, keepdims=True)
        sums[step, 1:2] = jnp.sum(second, axis=0, keepdims=True)

        def post(target, k):
            pltpu.make_async_remote_copy(
                sums.at[step], sums_in.at[step, k], sum_send.at[step], sum_recv.at[step],
                device_id=target, device_id_type=MESH).start()
        if ndom * nsub <= 64:
            for k, (a, b) in enumerate(others):
                post(peer(a, b), k)
        else:
            @pl.loop(1, ndom * nsub)
            def _(k):
                post((lax.rem(dom + k // nsub, ndom), lax.rem(sub + k % nsub, nsub)), k - 1)

    def finish_sums(step):
        pltpu.make_async_copy(sums_in.at[step], sums_in.at[step], sum_recv.at[step]).wait()
        total = sums[step] + jnp.sum(sums_in[step], axis=0)
        total = jnp.sum(total, axis=1, keepdims=True)
        return total[0:1], total[1:2]

    def dot(a, b, scale=None):
        total = None
        for i in span:
            term = a[i] * b[i]
            if scale is not None:
                term = term * scale[i]
            total = term if total is None else total + term
        return total

    for load in loads[:3]:
        load.wait()
    weight_plane = planes_v[3 * ORDER]
    count_plane = planes_v[3 * ORDER + 1]
    weight = [weight_plane * float(WEIGHTS[i]) for i in span]
    inv_mult = [count_plane * float(COUNT[i]) for i in span]

    phi = [level_v[i] for i in span]
    g0, g1, g2 = gradient(phi)
    loads[3].wait()
    advected = [
        phi[i] - advect_step * (velocity_v[0, i] * g0[i] + velocity_v[1, i] * g1[i]
                                + velocity_v[2, i] * g2[i]) for i in span]
    loads[4].wait()
    right = [weight[i] * source_v[i] for i in span]
    pl.semaphore_wait(barrier, len(near) if local_barrier else ndom * nsub - 1)
    fields = send(0, [advected, right], first_faces, first_edges, first_faces_in, first_edges_in)
    phi, right = receive(0, fields, first_faces_in, first_edges_in)
    phi = [phi[i] * inv_mult[i] for i in span]

    step = 0
    for sweep in range(SWEEPS):
        g0, g1, g2 = gradient(phi)
        if sweep == 0:
            scaled = [lax.rsqrt(jnp.maximum(
                g0[i] * g0[i] + g1[i] * g1[i] + g2[i] * g2[i], 1.0)) for i in span]
            normals = [[g[i] * scaled[i] for i in span] for g in (g0, g1, g2)]
        compress = [p * (1.0 - p) for p in phi]
        flux = [[interface_width * g[i] - compress[i] * normal[i] for i in span]
                for g, normal in zip((g0, g1, g2), normals)]
        change = assemble(step, divergence(flux, GRAD))
        step += 1
        phi = [phi[i] + reinit_step * change[i] * inv_mult[i] for i in span]

    for i in span:
        new_ref[i] = phi[i]
    weighted = [weight[i] * (1.0 / (1.0 + density_ratio * phi[i] * phi[i])) for i in span]
    squares = divergence([weighted] * 3, SQUARE)
    diagonal = assemble(step, [weight[i] + squares[i] for i in span])
    step += 1
    inverse = [1.0 / v for v in diagonal]

    def apply(step, sum_step, residual, precond):
        slopes = gradient(precond)
        parts = [[weighted[i] * g[i] for i in span] for g in slopes]
        mass = [weight[i] * precond[i] for i in span]
        energy = dot(precond, mass)
        for slope, part in zip(slopes, parts):
            energy = energy + dot(slope, part)
        begin_sums(sum_step, dot(residual, precond, inv_mult), energy)
        total = divergence(parts, TRANS)
        sent = begin(step, [mass[i] + total[i] for i in span])
        applied = finish(step, sent)
        return (applied,) + finish_sums(sum_step)

    residual = right
    precond = [residual[i] * inverse[i] for i in span]
    applied, norm_now, product = apply(step, 0, residual, precond)
    step += 1
    step_size = norm_now / product
    direction, image = precond, applied
    result = None
    for it in range(PITERS):
        moved = [step_size * d for d in direction]
        result = moved if result is None else [result[i] + moved[i] for i in span]
        residual = [residual[i] - step_size * image[i] for i in span]
        if it + 1 < PITERS:
            precond = [residual[i] * inverse[i] for i in span]
            applied, norm_next, product = apply(step, it + 1, residual, precond)
            step += 1
            ratio = norm_next / norm_now
            step_size = norm_next / (product - ratio * norm_next / step_size)
            direction = [precond[i] + ratio * direction[i] for i in span]
            image = [applied[i] + ratio * image[i] for i in span]
            norm_now = norm_next
    for i in span:
        pressure_ref[i] = result[i]
        correction_ref[i] = residual[i] * inverse[i]
    pltpu.make_async_copy(first_faces, first_faces, face_send.at[0]).wait()
    pltpu.make_async_copy(first_edges, first_edges, edge_send.at[0]).wait()
    for s in range(step):
        pltpu.make_async_copy(faces.at[s], faces.at[s], face_send.at[s + 1]).wait()
        pltpu.make_async_copy(edges.at[s], edges.at[s], edge_send.at[s + 1]).wait()
    for s in range(PITERS):
        pltpu.make_async_copy(sums_in.at[s], sums_in.at[s], sum_send.at[s]).wait()


def write_out(a_in, b_in, c_in, a_out, b_out, c_out, sem):
    copies = [pltpu.make_async_copy(src, dst, sem.at[i]) for i, (src, dst) in enumerate((
        (a_in, a_out), (b_in, b_out), (c_in, c_out)))]
    for copy in copies:
        copy.start()
    for copy in copies:
        copy.wait()


def solution(mesh):
    ndom, nsub = mesh.shape["dom"], mesh.shape["sub"]
    rounds = SWEEPS + 1 + PITERS
    local_barrier = max(ndom, nsub) // 2 <= SWEEPS + 3

    def local(level_set, velocity, source):
        assert level_set.shape[:2] == (ORDER, ORDER)
        lanes = level_set.shape[2]
        planes, wide = constants(lanes)
        tile = (ORDER, lanes)
        vmem = functools.partial(pltpu.VMEM, dtype=jnp.float32)
        others = ndom * nsub - 1
        dma = pltpu.SemaphoreType.DMA
        scratch = [
            vmem(level_set.shape), vmem(velocity.shape), vmem(source.shape),
            vmem(planes.shape), pltpu.VMEM(wide.shape, jnp.bfloat16),
            dma((5,)),
            dma((rounds + 1,)), dma((rounds + 1,)), dma((rounds + 1,)), dma((rounds + 1,)),
            dma((PITERS,)), dma((PITERS,)),
            vmem((4, 2) + tile), vmem((4, 2, 1, lanes)),
            vmem((4, 2) + tile), vmem((4, 2, 1, lanes)),
            vmem((rounds, 4, 1) + tile), vmem((rounds, 4, 1, 1, lanes)),
            vmem((rounds, 4, 1) + tile), vmem((rounds, 4, 1, 1, lanes)),
            vmem((PITERS, 2, lanes)), vmem((PITERS, others, 2, lanes)),
        ]
        any_space = pl.BlockSpec(memory_space=pl.ANY)
        hbm_space = pl.BlockSpec(memory_space=pltpu.HBM)
        out = jax.ShapeDtypeStruct(level_set.shape, jnp.float32)
        held = pltpu.VMEM(level_set.shape, jnp.float32)
        results = pl.pallas_call(
            functools.partial(kernel, ndom, nsub, local_barrier),
            out_shape=(held, held, held),
            in_specs=[hbm_space] * 5,
            out_specs=(pl.BlockSpec(memory_space=pltpu.VMEM),) * 3,
            scratch_shapes=scratch,
            compiler_params=pltpu.CompilerParams(
                collective_id=0, has_side_effects=True, vmem_limit_bytes=60 * 2**20),
        )(level_set, velocity, source, jnp.asarray(planes), jnp.asarray(wide))
        return pl.pallas_call(
            write_out,
            out_shape=(out, out, out),
            in_specs=[any_space] * 3,
            out_specs=(hbm_space,) * 3,
            scratch_shapes=[dma((3,))],
            compiler_params=pltpu.CompilerParams(vmem_limit_bytes=2**20),
        )(*results)

    return jax.shard_map(
        local,
        mesh=mesh,
        in_specs=(P("dom", "sub", None), P(None, "dom", "sub", None), P("dom", "sub", None)),
        out_specs=(P("dom", "sub", None), P("dom", "sub", None), P("dom", "sub", None)),
        check_vma=False,
    )
```

```python
import functools

import jax
import jax.numpy as jnp
import numpy as np
from jax import lax
from jax.experimental import pallas as pl
from jax.experimental.pallas import tpu as pltpu
from jax.sharding import PartitionSpec as P

SWEEPS = 2
PITERS = 2
MESH = pl.DeviceIdType.MESH


gll_nodes = [
    -1.0,
    -0.8717401485096066,
    -0.5917001814331423,
    -0.2092992179024789,
    0.2092992179024789,
    0.5917001814331423,
    0.8717401485096066,
    1.0,
]
advect_step = 0.05
reinit_step = 0.02
interface_width = 0.1
density_ratio = 9.0
ORDER = 8
GRAD, TRANS, SQUARE = 0, 1, 2


def tables():
    node_points = np.array(gll_nodes)
    poly_order = 7
    values_prev = np.ones(8)
    values_now = node_points.copy()
    for degree in range(1, poly_order):
        values_next = ((2 * degree + 1) * node_points * values_now - degree * values_prev) / (
            degree + 1
        )
        values_prev, values_now = (values_now, values_next)
    matrix = np.zeros((8, 8))
    for line in range(8):
        for column in range(8):
            if line != column:
                matrix[line, column] = values_now[line] / (
                    values_now[column] * (node_points[line] - node_points[column])
                )
    matrix[0, 0] = -poly_order * (poly_order + 1) / 4.0
    matrix[7, 7] = poly_order * (poly_order + 1) / 4.0
    weights = 2.0 / (poly_order * (poly_order + 1) * values_now**2)
    return (matrix, weights)


MATRIX, WEIGHTS = tables()
KINDS = (MATRIX, MATRIX.T, (MATRIX * MATRIX).T)
COUNT = np.array([0.5, 1.0, 1.0, 1.0, 1.0, 1.0, 1.0, 0.5])


def constants(lanes):
    rows = np.arange(ORDER)
    planes = []
    for matrix in KINDS:
        for shift in range(ORDER):
            column = matrix[rows, (rows - shift) % ORDER]
            planes.append(np.broadcast_to(column[:, None], (ORDER, lanes)))
    repeats = lanes // ORDER
    planes.append(WEIGHTS[:, None] * np.tile(WEIGHTS, repeats)[None, :])
    planes.append(COUNT[:, None] * np.tile(COUNT, repeats)[None, :])
    planes = np.stack(planes).astype(np.float32)
    wide = []
    for matrix in KINDS:
        full = np.kron(np.eye(repeats), matrix.T).astype(np.float32)
        high = full.astype(jnp.bfloat16)
        low = (full - high.astype(np.float32)).astype(jnp.bfloat16)
        wide.append(np.concatenate([high, low], axis=1))
    return planes, np.stack(wide)


def along_first(values, kind):
    matrix = KINDS[kind]
    half = ORDER // 2
    flip = -1.0 if kind != SQUARE else 1.0
    even = [values[i] + values[ORDER - 1 - i] for i in range(half)]
    odd = [values[i] - values[ORDER - 1 - i] for i in range(half)]
    front, back = [], []
    for j in range(half):
        even_sum = odd_sum = None
        for i in range(half):
            ce = float(0.5 * (matrix[j, i] + matrix[j, ORDER - 1 - i]))
            co = float(0.5 * (matrix[j, i] - matrix[j, ORDER - 1 - i]))
            even_sum = even[i] * ce if even_sum is None else even_sum + even[i] * ce
            odd_sum = odd[i] * co if odd_sum is None else odd_sum + odd[i] * co
        front.append(even_sum + odd_sum)
        back.append(flip * (even_sum - odd_sum))
    return front + back[::-1]


def kernel(ndom, nsub, local_barrier, level_ref, velocity_ref, source_ref, planes_ref, wide_ref,
           new_ref, pressure_ref, correction_ref, *scratch):
    (level_v, velocity_v, source_v, planes_v, wide_v, in_sem,
     face_send, face_recv, edge_send, edge_recv, sum_send, sum_recv,
     faces, edges, faces_in, edges_in, sums, sums_in) = scratch
    dom, sub = lax.axis_index("dom"), lax.axis_index("sub")

    def peer(a, b):
        return (lax.rem(dom + a % ndom, ndom), lax.rem(sub + b % nsub, nsub))

    loads = [
        pltpu.make_async_copy(src, dst, in_sem.at[i])
        for i, (src, dst) in enumerate((
            (level_ref, level_v), (planes_ref, planes_v), (wide_ref, wide_v),
            (velocity_ref, velocity_v), (source_ref, source_v)))
    ]
    barrier = pltpu.get_barrier_semaphore()
    near = [(a, b) for a in (-1, 1, 0) for b in (-1, 1, 0) if a or b]
    if local_barrier:
        for a, b in near:
            pl.semaphore_signal(barrier, inc=1, device_id=peer(a, b), device_id_type=MESH)
    else:
        @pl.loop(1, ndom * nsub)
        def _(k):
            target = (lax.rem(dom + k // nsub, ndom), lax.rem(sub + k % nsub, nsub))
            pl.semaphore_signal(barrier, inc=1, device_id=target, device_id_type=MESH)
    for load in loads:
        load.start()

    shape = level_v.shape[1:]
    lane = lax.broadcasted_iota(jnp.int32, shape, 1) % ORDER
    row = lax.broadcasted_iota(jnp.int32, shape, 0)
    lane_first, lane_last = lane == 0, lane == ORDER - 1
    row_first, row_last = row == 0, row == ORDER - 1
    lanes = shape[1]
    span = range(ORDER)

    def fold_lanes(v):
        lower = pltpu.roll(v, 1, 1)
        upper = pltpu.roll(v, lanes - 1, 1)
        return v + jnp.where(lane_last, upper, jnp.where(lane_first, lower, 0.0))

    def along_second(values, kind):
        result = []
        for v in values:
            total = v * planes_v[kind * ORDER]
            for shift in range(1, ORDER):
                total = total + pltpu.roll(v, shift, 0) * planes_v[kind * ORDER + shift]
            result.append(total)
        return result

    def along_third(values, kind):
        stacked = jnp.concatenate(values, axis=0)
        high = stacked.astype(jnp.bfloat16)
        low = (stacked - high.astype(jnp.float32)).astype(jnp.bfloat16)
        out = jnp.dot(jnp.concatenate([high, low], axis=0), wide_v[kind],
                      preferred_element_type=jnp.float32)
        n = ORDER * ORDER
        total = out[:n, :lanes] + (out[:n, lanes:] + out[n:, :lanes])
        return [total[i * ORDER:(i + 1) * ORDER] for i in span]

    def gradient(values):
        third = along_third(values, GRAD)
        return along_first(values, GRAD), along_second(values, GRAD), third

    def divergence(parts, kind):
        third = along_third(parts[2], kind)
        first, second = along_first(parts[0], kind), along_second(parts[1], kind)
        return [(first[i] + second[i]) + third[i] for i in span]

    def begin(step, field):
        face_out, edge_out = faces.at[step], edges.at[step]
        last, first = fold_lanes(field[ORDER - 1]), fold_lanes(field[0])
        face_out[0], face_out[1] = last, first
        edge_out[0], edge_out[1] = last[ORDER - 1:], last[:1]
        edge_out[2], edge_out[3] = first[ORDER - 1:], first[:1]

        def post_face(i, a, b):
            pltpu.make_async_remote_copy(
                face_out.at[i], faces_in.at[step, i], face_send.at[step], face_recv.at[step],
                device_id=peer(a, b), device_id_type=MESH).start()

        for i, (a, b) in enumerate(((1, 1), (1, -1), (-1, 1), (-1, -1))):
            pltpu.make_async_remote_copy(
                edge_out.at[i], edges_in.at[step, i], edge_send.at[step], edge_recv.at[step],
                device_id=peer(a, b), device_id_type=MESH).start()
        post_face(0, 1, 0)
        post_face(1, -1, 0)
        face_out[2] = fold_lanes(jnp.concatenate([v[ORDER - 1:] for v in field], axis=0))
        face_out[3] = fold_lanes(jnp.concatenate([v[:1] for v in field], axis=0))
        post_face(2, 0, 1)
        post_face(3, 0, -1)
        return [first] + [fold_lanes(v) for v in field[1:-1]] + [last]

    def finish(step, field):
        face_in, edge_in = faces_in.at[step], edges_in.at[step]
        pltpu.make_async_copy(face_in, face_in, face_recv.at[step]).wait()
        pltpu.make_async_copy(edge_in, edge_in, edge_recv.at[step]).wait()
        result = list(field)
        for i, at in enumerate((0, ORDER - 1)):
            result[at] = result[at] + face_in[i] + jnp.where(
                row_first, edge_in[2 * i], jnp.where(row_last, edge_in[2 * i + 1], 0.0))
        for i in span:
            result[i] = result[i] + jnp.where(
                row_first, face_in[2, i:i + 1], jnp.where(row_last, face_in[3, i:i + 1], 0.0))
        return result

    def assemble(step, field):
        return finish(step, begin(step, field))

    hops = sorted(range(ndom), key=lambda a: min(a, ndom - a) or ndom)
    others = [(a, b) for a in hops for b in (2, 1, 3, 0) if a or b] if nsub == 4 else [
        (a, b) for a in hops for b in range(nsub) if a or b]

    def begin_sums(step, first, second):
        sums[step, 0:1] = jnp.sum(first, axis=0, keepdims=True)
        sums[step, 1:2] = jnp.sum(second, axis=0, keepdims=True)

        def post(target, k):
            pltpu.make_async_remote_copy(
                sums.at[step], sums_in.at[step, k], sum_send.at[step], sum_recv.at[step],
                device_id=target, device_id_type=MESH).start()
        if ndom * nsub <= 64:
            for k, (a, b) in enumerate(others):
                post(peer(a, b), k)
        else:
            @pl.loop(1, ndom * nsub)
            def _(k):
                post((lax.rem(dom + k // nsub, ndom), lax.rem(sub + k % nsub, nsub)), k - 1)

    def finish_sums(step):
        pltpu.make_async_copy(sums_in.at[step], sums_in.at[step], sum_recv.at[step]).wait()
        total = sums[step] + jnp.sum(sums_in[step], axis=0)
        total = jnp.sum(total, axis=1, keepdims=True)
        return total[0:1], total[1:2]

    def dot(a, b, scale=None):
        total = None
        for i in span:
            term = a[i] * b[i]
            if scale is not None:
                term = term * scale[i]
            total = term if total is None else total + term
        return total

    for load in loads[:3]:
        load.wait()
    weight_plane = planes_v[3 * ORDER]
    count_plane = planes_v[3 * ORDER + 1]
    weight = [weight_plane * float(WEIGHTS[i]) for i in span]
    inv_mult = [count_plane * float(COUNT[i]) for i in span]

    phi = [level_v[i] for i in span]
    g0, g1, g2 = gradient(phi)
    loads[3].wait()
    advected = [
        phi[i] - advect_step * (velocity_v[0, i] * g0[i] + velocity_v[1, i] * g1[i]
                                + velocity_v[2, i] * g2[i]) for i in span]
    pl.semaphore_wait(barrier, len(near) if local_barrier else ndom * nsub - 1)
    sent = begin(0, advected)
    loads[4].wait()
    sent_right = begin(1, [weight[i] * source_v[i] for i in span])
    phi = finish(0, sent)
    phi = [phi[i] * inv_mult[i] for i in span]

    step = 2
    for sweep in range(SWEEPS):
        g0, g1, g2 = gradient(phi)
        if sweep == 0:
            scaled = [lax.rsqrt(jnp.maximum(
                g0[i] * g0[i] + g1[i] * g1[i] + g2[i] * g2[i], 1.0)) for i in span]
            normals = [[g[i] * scaled[i] for i in span] for g in (g0, g1, g2)]
        compress = [p * (1.0 - p) for p in phi]
        flux = [[interface_width * g[i] - compress[i] * normal[i] for i in span]
                for g, normal in zip((g0, g1, g2), normals)]
        change = assemble(step, divergence(flux, GRAD))
        step += 1
        phi = [phi[i] + reinit_step * change[i] * inv_mult[i] for i in span]

    for i in span:
        new_ref[i] = phi[i]
    weighted = [weight[i] * (1.0 / (1.0 + density_ratio * phi[i] * phi[i])) for i in span]
    squares = divergence([weighted] * 3, SQUARE)
    diagonal = assemble(step, [weight[i] + squares[i] for i in span])
    step += 1
    inverse = [1.0 / v for v in diagonal]

    def apply(step, sum_step, residual, precond):
        slopes = gradient(precond)
        parts = [[weighted[i] * g[i] for i in span] for g in slopes]
        mass = [weight[i] * precond[i] for i in span]
        energy = dot(precond, mass)
        for slope, part in zip(slopes, parts):
            energy = energy + dot(slope, part)
        begin_sums(sum_step, dot(residual, precond, inv_mult), energy)
        total = divergence(parts, TRANS)
        sent = begin(step, [mass[i] + total[i] for i in span])
        applied = finish(step, sent)
        return (applied,) + finish_sums(sum_step)

    residual = finish(1, sent_right)
    precond = [residual[i] * inverse[i] for i in span]
    applied, norm_now, product = apply(step, 0, residual, precond)
    step += 1
    step_size = norm_now / product
    direction, image = precond, applied
    result = None
    for it in range(PITERS):
        moved = [step_size * d for d in direction]
        result = moved if result is None else [result[i] + moved[i] for i in span]
        residual = [residual[i] - step_size * image[i] for i in span]
        if it + 1 < PITERS:
            precond = [residual[i] * inverse[i] for i in span]
            applied, norm_next, product = apply(step, it + 1, residual, precond)
            step += 1
            ratio = norm_next / norm_now
            step_size = norm_next / (product - ratio * norm_next / step_size)
            direction = [precond[i] + ratio * direction[i] for i in span]
            image = [applied[i] + ratio * image[i] for i in span]
            norm_now = norm_next
    for i in span:
        pressure_ref[i] = result[i]
        correction_ref[i] = residual[i] * inverse[i]
    for s in range(step):
        pltpu.make_async_copy(faces.at[s], faces.at[s], face_send.at[s]).wait()
        pltpu.make_async_copy(edges.at[s], edges.at[s], edge_send.at[s]).wait()
    for s in range(PITERS):
        pltpu.make_async_copy(sums_in.at[s], sums_in.at[s], sum_send.at[s]).wait()


def write_out(a_in, b_in, c_in, a_out, b_out, c_out, sem):
    copies = [pltpu.make_async_copy(src, dst, sem.at[i]) for i, (src, dst) in enumerate((
        (a_in, a_out), (b_in, b_out), (c_in, c_out)))]
    for copy in copies:
        copy.start()
    for copy in copies:
        copy.wait()


def solution(mesh):
    ndom, nsub = mesh.shape["dom"], mesh.shape["sub"]
    rounds = SWEEPS + 3 + PITERS
    local_barrier = max(ndom, nsub) // 2 <= SWEEPS + 3

    def local(level_set, velocity, source):
        assert level_set.shape[:2] == (ORDER, ORDER)
        lanes = level_set.shape[2]
        planes, wide = constants(lanes)
        tile = (ORDER, lanes)
        vmem = functools.partial(pltpu.VMEM, dtype=jnp.float32)
        others = ndom * nsub - 1
        dma = pltpu.SemaphoreType.DMA
        scratch = [
            vmem(level_set.shape), vmem(velocity.shape), vmem(source.shape),
            vmem(planes.shape), pltpu.VMEM(wide.shape, jnp.bfloat16),
            dma((5,)),
            dma((rounds,)), dma((rounds,)), dma((rounds,)), dma((rounds,)),
            dma((PITERS,)), dma((PITERS,)),
            vmem((rounds, 4) + tile), vmem((rounds, 4, 1, lanes)),
            vmem((rounds, 4) + tile), vmem((rounds, 4, 1, lanes)),
            vmem((PITERS, 2, lanes)), vmem((PITERS, others, 2, lanes)),
        ]
        any_space = pl.BlockSpec(memory_space=pl.ANY)
        hbm_space = pl.BlockSpec(memory_space=pltpu.HBM)
        out = jax.ShapeDtypeStruct(level_set.shape, jnp.float32)
        held = pltpu.VMEM(level_set.shape, jnp.float32)
        results = pl.pallas_call(
            functools.partial(kernel, ndom, nsub, local_barrier),
            out_shape=(held, held, held),
            in_specs=[hbm_space] * 5,
            out_specs=(pl.BlockSpec(memory_space=pltpu.VMEM),) * 3,
            scratch_shapes=scratch,
            compiler_params=pltpu.CompilerParams(
                collective_id=0, has_side_effects=True, vmem_limit_bytes=60 * 2**20),
        )(level_set, velocity, source, jnp.asarray(planes), jnp.asarray(wide))
        return pl.pallas_call(
            write_out,
            out_shape=(out, out, out),
            in_specs=[any_space] * 3,
            out_specs=(hbm_space,) * 3,
            scratch_shapes=[dma((3,))],
            compiler_params=pltpu.CompilerParams(vmem_limit_bytes=2**20),
        )(*results)

    return jax.shard_map(
        local,
        mesh=mesh,
        in_specs=(P("dom", "sub", None), P(None, "dom", "sub", None), P("dom", "sub", None)),
        out_specs=(P("dom", "sub", None), P("dom", "sub", None), P("dom", "sub", None)),
        check_vma=False,
    )
```

```python
import functools

import jax
import jax.numpy as jnp
import numpy as np
from jax import lax
from jax.experimental import pallas as pl
from jax.experimental.pallas import tpu as pltpu
from jax.sharding import PartitionSpec as P

SWEEPS = 2
PITERS = 2
MESH = pl.DeviceIdType.MESH


gll_nodes = [
    -1.0,
    -0.8717401485096066,
    -0.5917001814331423,
    -0.2092992179024789,
    0.2092992179024789,
    0.5917001814331423,
    0.8717401485096066,
    1.0,
]
advect_step = 0.05
reinit_step = 0.02
interface_width = 0.1
density_ratio = 9.0
ORDER = 8
GRAD, TRANS, SQUARE = 0, 1, 2


def tables():
    node_points = np.array(gll_nodes)
    poly_order = 7
    values_prev = np.ones(8)
    values_now = node_points.copy()
    for degree in range(1, poly_order):
        values_next = ((2 * degree + 1) * node_points * values_now - degree * values_prev) / (
            degree + 1
        )
        values_prev, values_now = (values_now, values_next)
    matrix = np.zeros((8, 8))
    for line in range(8):
        for column in range(8):
            if line != column:
                matrix[line, column] = values_now[line] / (
                    values_now[column] * (node_points[line] - node_points[column])
                )
    matrix[0, 0] = -poly_order * (poly_order + 1) / 4.0
    matrix[7, 7] = poly_order * (poly_order + 1) / 4.0
    weights = 2.0 / (poly_order * (poly_order + 1) * values_now**2)
    return (matrix, weights)


MATRIX, WEIGHTS = tables()
KINDS = (MATRIX, MATRIX.T, (MATRIX * MATRIX).T)
COUNT = np.array([0.5, 1.0, 1.0, 1.0, 1.0, 1.0, 1.0, 0.5])


def constants(lanes):
    rows = np.arange(ORDER)
    planes = []
    for matrix in KINDS:
        for shift in range(ORDER):
            column = matrix[rows, (rows - shift) % ORDER]
            planes.append(np.broadcast_to(column[:, None], (ORDER, lanes)))
    repeats = lanes // ORDER
    planes.append(WEIGHTS[:, None] * np.tile(WEIGHTS, repeats)[None, :])
    planes.append(COUNT[:, None] * np.tile(COUNT, repeats)[None, :])
    planes = np.stack(planes).astype(np.float32)
    wide = []
    for matrix in KINDS:
        full = np.kron(np.eye(repeats), matrix.T).astype(np.float32)
        high = full.astype(jnp.bfloat16)
        low = (full - high.astype(np.float32)).astype(jnp.bfloat16)
        wide.append(np.concatenate([high, low], axis=1))
    return planes, np.stack(wide)


def along_first(values, kind):
    matrix = KINDS[kind]
    half = ORDER // 2
    flip = -1.0 if kind != SQUARE else 1.0
    even = [values[i] + values[ORDER - 1 - i] for i in range(half)]
    odd = [values[i] - values[ORDER - 1 - i] for i in range(half)]
    front, back = [], []
    for j in range(half):
        even_sum = odd_sum = None
        for i in range(half):
            ce = float(0.5 * (matrix[j, i] + matrix[j, ORDER - 1 - i]))
            co = float(0.5 * (matrix[j, i] - matrix[j, ORDER - 1 - i]))
            even_sum = even[i] * ce if even_sum is None else even_sum + even[i] * ce
            odd_sum = odd[i] * co if odd_sum is None else odd_sum + odd[i] * co
        front.append(even_sum + odd_sum)
        back.append(flip * (even_sum - odd_sum))
    return front + back[::-1]


def kernel(ndom, nsub, local_barrier, level_ref, velocity_ref, source_ref, planes_ref, wide_ref,
           new_ref, pressure_ref, correction_ref, *scratch):
    (level_v, velocity_v, source_v, planes_v, wide_v, in_sem,
     face_send, face_recv, edge_send, edge_recv, sum_send, sum_recv,
     faces, edges, faces_in, edges_in, sums, sums_in) = scratch
    dom, sub = lax.axis_index("dom"), lax.axis_index("sub")

    def peer(a, b):
        return (lax.rem(dom + a % ndom, ndom), lax.rem(sub + b % nsub, nsub))

    loads = [
        pltpu.make_async_copy(src, dst, in_sem.at[i])
        for i, (src, dst) in enumerate((
            (level_ref, level_v), (planes_ref, planes_v), (wide_ref, wide_v),
            (velocity_ref, velocity_v), (source_ref, source_v)))
    ]
    barrier = pltpu.get_barrier_semaphore()
    near = [(a, b) for a in (-1, 1, 0) for b in (-1, 1, 0) if a or b]
    if local_barrier:
        for a, b in near:
            pl.semaphore_signal(barrier, inc=1, device_id=peer(a, b), device_id_type=MESH)
    else:
        @pl.loop(1, ndom * nsub)
        def _(k):
            target = (lax.rem(dom + k // nsub, ndom), lax.rem(sub + k % nsub, nsub))
            pl.semaphore_signal(barrier, inc=1, device_id=target, device_id_type=MESH)
    for load in loads:
        load.start()

    shape = level_v.shape[1:]
    lane = lax.broadcasted_iota(jnp.int32, shape, 1) % ORDER
    row = lax.broadcasted_iota(jnp.int32, shape, 0)
    lane_first, lane_last = lane == 0, lane == ORDER - 1
    row_first, row_last = row == 0, row == ORDER - 1
    lanes = shape[1]
    span = range(ORDER)

    def fold_lanes(v):
        lower = pltpu.roll(v, 1, 1)
        upper = pltpu.roll(v, lanes - 1, 1)
        return v + jnp.where(lane_last, upper, jnp.where(lane_first, lower, 0.0))

    def along_second(values, kind):
        result = []
        for v in values:
            total = v * planes_v[kind * ORDER]
            for shift in range(1, ORDER):
                total = total + pltpu.roll(v, shift, 0) * planes_v[kind * ORDER + shift]
            result.append(total)
        return result

    def along_third(values, kind):
        stacked = jnp.concatenate(values, axis=0)
        high = stacked.astype(jnp.bfloat16)
        low = (stacked - high.astype(jnp.float32)).astype(jnp.bfloat16)
        out = jnp.dot(jnp.concatenate([high, low], axis=0), wide_v[kind],
                      preferred_element_type=jnp.float32)
        n = ORDER * ORDER
        total = out[:n, :lanes] + (out[:n, lanes:] + out[n:, :lanes])
        return [total[i * ORDER:(i + 1) * ORDER] for i in span]

    def gradient(values):
        third = along_third(values, GRAD)
        return along_first(values, GRAD), along_second(values, GRAD), third

    def divergence(parts, kind):
        third = along_third(parts[2], kind)
        first, second = along_first(parts[0], kind), along_second(parts[1], kind)
        return [(first[i] + second[i]) + third[i] for i in span]

    upper = dom // (ndom // 2)
    ways = ((1 - upper, lax.rem(dom + 2 * upper - 1 + ndom, ndom)),
            (upper, lax.rem(dom - 2 * upper + 1 + ndom, ndom)))

    def begin(step, field):
        face_out, edge_out = faces.at[step], edges.at[step]
        last, first = fold_lanes(field[ORDER - 1]), fold_lanes(field[0])
        face_out[0], face_out[1] = last, first
        edge_out[0], edge_out[1] = last[ORDER - 1:], last[:1]
        edge_out[2], edge_out[3] = first[ORDER - 1:], first[:1]

        def post(out, into, slot, sends, receives, target):
            pltpu.make_async_remote_copy(
                out.at[slot], into.at[step, slot], sends.at[step], receives.at[step],
                device_id=target, device_id_type=MESH).start()

        for slot, beside in ways:
            for j, b in enumerate((1, -1)):
                post(edge_out, edges_in, 2 * slot + j, edge_send, edge_recv,
                     (beside, lax.rem(sub + b % nsub, nsub)))
            post(face_out, faces_in, slot, face_send, face_recv, (beside, sub))
        face_out[2] = fold_lanes(jnp.concatenate([v[ORDER - 1:] for v in field], axis=0))
        face_out[3] = fold_lanes(jnp.concatenate([v[:1] for v in field], axis=0))
        post(face_out, faces_in, 2, face_send, face_recv, peer(0, 1))
        post(face_out, faces_in, 3, face_send, face_recv, peer(0, -1))
        return [first] + [fold_lanes(v) for v in field[1:-1]] + [last]

    def finish(step, field):
        face_in, edge_in = faces_in.at[step], edges_in.at[step]
        pltpu.make_async_copy(face_in, face_in, face_recv.at[step]).wait()
        pltpu.make_async_copy(edge_in, edge_in, edge_recv.at[step]).wait()
        result = list(field)
        for i, at in enumerate((0, ORDER - 1)):
            result[at] = result[at] + face_in[i] + jnp.where(
                row_first, edge_in[2 * i], jnp.where(row_last, edge_in[2 * i + 1], 0.0))
        for i in span:
            result[i] = result[i] + jnp.where(
                row_first, face_in[2, i:i + 1], jnp.where(row_last, face_in[3, i:i + 1], 0.0))
        return result

    def assemble(step, field):
        return finish(step, begin(step, field))

    hops = sorted(range(ndom), key=lambda a: min(a, ndom - a) or ndom)
    others = [(a, b) for a in hops for b in (2, 1, 3, 0) if a or b] if nsub == 4 else [
        (a, b) for a in hops for b in range(nsub) if a or b]

    def begin_sums(step, first, second):
        sums[step, 0:1] = jnp.sum(first, axis=0, keepdims=True)
        sums[step, 1:2] = jnp.sum(second, axis=0, keepdims=True)

        def post(target, k):
            pltpu.make_async_remote_copy(
                sums.at[step], sums_in.at[step, k], sum_send.at[step], sum_recv.at[step],
                device_id=target, device_id_type=MESH).start()
        if ndom * nsub <= 64:
            for k, (a, b) in enumerate(others):
                post(peer(a, b), k)
        else:
            @pl.loop(1, ndom * nsub)
            def _(k):
                post((lax.rem(dom + k // nsub, ndom), lax.rem(sub + k % nsub, nsub)), k - 1)

    def finish_sums(step):
        pltpu.make_async_copy(sums_in.at[step], sums_in.at[step], sum_recv.at[step]).wait()
        total = sums[step] + jnp.sum(sums_in[step], axis=0)
        total = jnp.sum(total, axis=1, keepdims=True)
        return total[0:1], total[1:2]

    def dot(a, b, scale=None):
        total = None
        for i in span:
            term = a[i] * b[i]
            if scale is not None:
                term = term * scale[i]
            total = term if total is None else total + term
        return total

    for load in loads[:3]:
        load.wait()
    weight_plane = planes_v[3 * ORDER]
    count_plane = planes_v[3 * ORDER + 1]
    weight = [weight_plane * float(WEIGHTS[i]) for i in span]
    inv_mult = [count_plane * float(COUNT[i]) for i in span]

    phi = [level_v[i] for i in span]
    g0, g1, g2 = gradient(phi)
    loads[3].wait()
    advected = [
        phi[i] - advect_step * (velocity_v[0, i] * g0[i] + velocity_v[1, i] * g1[i]
                                + velocity_v[2, i] * g2[i]) for i in span]
    pl.semaphore_wait(barrier, len(near) if local_barrier else ndom * nsub - 1)
    sent = begin(0, advected)
    loads[4].wait()
    sent_right = begin(1, [weight[i] * source_v[i] for i in span])
    phi = finish(0, sent)
    phi = [phi[i] * inv_mult[i] for i in span]

    step = 2
    for sweep in range(SWEEPS):
        g0, g1, g2 = gradient(phi)
        if sweep == 0:
            scaled = [lax.rsqrt(jnp.maximum(
                g0[i] * g0[i] + g1[i] * g1[i] + g2[i] * g2[i], 1.0)) for i in span]
            normals = [[g[i] * scaled[i] for i in span] for g in (g0, g1, g2)]
        compress = [p * (1.0 - p) for p in phi]
        flux = [[interface_width * g[i] - compress[i] * normal[i] for i in span]
                for g, normal in zip((g0, g1, g2), normals)]
        change = assemble(step, divergence(flux, GRAD))
        step += 1
        phi = [phi[i] + reinit_step * change[i] * inv_mult[i] for i in span]

    for i in span:
        new_ref[i] = phi[i]
    weighted = [weight[i] * (1.0 / (1.0 + density_ratio * phi[i] * phi[i])) for i in span]
    squares = divergence([weighted] * 3, SQUARE)
    diagonal = assemble(step, [weight[i] + squares[i] for i in span])
    step += 1
    inverse = [1.0 / v for v in diagonal]

    def apply(step, sum_step, residual, precond):
        slopes = gradient(precond)
        parts = [[weighted[i] * g[i] for i in span] for g in slopes]
        mass = [weight[i] * precond[i] for i in span]
        energy = dot(precond, mass)
        for slope, part in zip(slopes, parts):
            energy = energy + dot(slope, part)
        begin_sums(sum_step, dot(residual, precond, inv_mult), energy)
        total = divergence(parts, TRANS)
        sent = begin(step, [mass[i] + total[i] for i in span])
        applied = finish(step, sent)
        return (applied,) + finish_sums(sum_step)

    residual = finish(1, sent_right)
    precond = [residual[i] * inverse[i] for i in span]
    applied, norm_now, product = apply(step, 0, residual, precond)
    step += 1
    step_size = norm_now / product
    direction, image = precond, applied
    result = None
    for it in range(PITERS):
        moved = [step_size * d for d in direction]
        result = moved if result is None else [result[i] + moved[i] for i in span]
        residual = [residual[i] - step_size * image[i] for i in span]
        if it + 1 < PITERS:
            precond = [residual[i] * inverse[i] for i in span]
            applied, norm_next, product = apply(step, it + 1, residual, precond)
            step += 1
            ratio = norm_next / norm_now
            step_size = norm_next / (product - ratio * norm_next / step_size)
            direction = [precond[i] + ratio * direction[i] for i in span]
            image = [applied[i] + ratio * image[i] for i in span]
            norm_now = norm_next
    for i in span:
        pressure_ref[i] = result[i]
        correction_ref[i] = residual[i] * inverse[i]
    for s in range(step):
        pltpu.make_async_copy(faces.at[s], faces.at[s], face_send.at[s]).wait()
        pltpu.make_async_copy(edges.at[s], edges.at[s], edge_send.at[s]).wait()
    for s in range(PITERS):
        pltpu.make_async_copy(sums_in.at[s], sums_in.at[s], sum_send.at[s]).wait()


def write_out(a_in, b_in, c_in, a_out, b_out, c_out, sem):
    copies = [pltpu.make_async_copy(src, dst, sem.at[i]) for i, (src, dst) in enumerate((
        (a_in, a_out), (b_in, b_out), (c_in, c_out)))]
    for copy in copies:
        copy.start()
    for copy in copies:
        copy.wait()


def solution(mesh):
    ndom, nsub = mesh.shape["dom"], mesh.shape["sub"]
    rounds = SWEEPS + 3 + PITERS
    local_barrier = max(ndom, nsub) // 2 <= SWEEPS + 3

    def local(level_set, velocity, source):
        assert level_set.shape[:2] == (ORDER, ORDER)
        lanes = level_set.shape[2]
        planes, wide = constants(lanes)
        tile = (ORDER, lanes)
        vmem = functools.partial(pltpu.VMEM, dtype=jnp.float32)
        others = ndom * nsub - 1
        dma = pltpu.SemaphoreType.DMA
        scratch = [
            vmem(level_set.shape), vmem(velocity.shape), vmem(source.shape),
            vmem(planes.shape), pltpu.VMEM(wide.shape, jnp.bfloat16),
            dma((5,)),
            dma((rounds,)), dma((rounds,)), dma((rounds,)), dma((rounds,)),
            dma((PITERS,)), dma((PITERS,)),
            vmem((rounds, 4) + tile), vmem((rounds, 4, 1, lanes)),
            vmem((rounds, 4) + tile), vmem((rounds, 4, 1, lanes)),
            vmem((PITERS, 2, lanes)), vmem((PITERS, others, 2, lanes)),
        ]
        any_space = pl.BlockSpec(memory_space=pl.ANY)
        hbm_space = pl.BlockSpec(memory_space=pltpu.HBM)
        out = jax.ShapeDtypeStruct(level_set.shape, jnp.float32)
        held = pltpu.VMEM(level_set.shape, jnp.float32)
        results = pl.pallas_call(
            functools.partial(kernel, ndom, nsub, local_barrier),
            out_shape=(held, held, held),
            in_specs=[hbm_space] * 5,
            out_specs=(pl.BlockSpec(memory_space=pltpu.VMEM),) * 3,
            scratch_shapes=scratch,
            compiler_params=pltpu.CompilerParams(
                collective_id=0, has_side_effects=True, vmem_limit_bytes=60 * 2**20),
        )(level_set, velocity, source, jnp.asarray(planes), jnp.asarray(wide))
        return pl.pallas_call(
            write_out,
            out_shape=(out, out, out),
            in_specs=[any_space] * 3,
            out_specs=(hbm_space,) * 3,
            scratch_shapes=[dma((3,))],
            compiler_params=pltpu.CompilerParams(vmem_limit_bytes=2**20),
        )(*results)

    return jax.shard_map(
        local,
        mesh=mesh,
        in_specs=(P("dom", "sub", None), P(None, "dom", "sub", None), P("dom", "sub", None)),
        out_specs=(P("dom", "sub", None), P("dom", "sub", None), P("dom", "sub", None)),
        check_vma=False,
    )
```

```python
import functools

import jax
import jax.numpy as jnp
import numpy as np
from jax import lax
from jax.experimental import pallas as pl
from jax.experimental.pallas import tpu as pltpu
from jax.sharding import PartitionSpec as P

SWEEPS = 2
PITERS = 2
MESH = pl.DeviceIdType.MESH


gll_nodes = [
    -1.0,
    -0.8717401485096066,
    -0.5917001814331423,
    -0.2092992179024789,
    0.2092992179024789,
    0.5917001814331423,
    0.8717401485096066,
    1.0,
]
advect_step = 0.05
reinit_step = 0.02
interface_width = 0.1
density_ratio = 9.0
ORDER = 8
GRAD, TRANS, SQUARE = 0, 1, 2


def tables():
    node_points = np.array(gll_nodes)
    poly_order = 7
    values_prev = np.ones(8)
    values_now = node_points.copy()
    for degree in range(1, poly_order):
        values_next = ((2 * degree + 1) * node_points * values_now - degree * values_prev) / (
            degree + 1
        )
        values_prev, values_now = (values_now, values_next)
    matrix = np.zeros((8, 8))
    for line in range(8):
        for column in range(8):
            if line != column:
                matrix[line, column] = values_now[line] / (
                    values_now[column] * (node_points[line] - node_points[column])
                )
    matrix[0, 0] = -poly_order * (poly_order + 1) / 4.0
    matrix[7, 7] = poly_order * (poly_order + 1) / 4.0
    weights = 2.0 / (poly_order * (poly_order + 1) * values_now**2)
    return (matrix, weights)


MATRIX, WEIGHTS = tables()
KINDS = (MATRIX, MATRIX.T, (MATRIX * MATRIX).T)
COUNT = np.array([0.5, 1.0, 1.0, 1.0, 1.0, 1.0, 1.0, 0.5])


def constants(lanes):
    rows = np.arange(ORDER)
    planes = []
    for matrix in KINDS:
        for shift in range(ORDER):
            column = matrix[rows, (rows - shift) % ORDER]
            planes.append(np.broadcast_to(column[:, None], (ORDER, lanes)))
    repeats = lanes // ORDER
    planes.append(WEIGHTS[:, None] * np.tile(WEIGHTS, repeats)[None, :])
    planes.append(COUNT[:, None] * np.tile(COUNT, repeats)[None, :])
    planes = np.stack(planes).astype(np.float32)
    wide = []
    for matrix in KINDS:
        full = np.kron(np.eye(repeats), matrix.T).astype(np.float32)
        high = full.astype(jnp.bfloat16)
        low = (full - high.astype(np.float32)).astype(jnp.bfloat16)
        wide.append(np.concatenate([high, low], axis=1))
    return planes, np.stack(wide)


def along_first(values, kind):
    matrix = KINDS[kind]
    half = ORDER // 2
    flip = -1.0 if kind != SQUARE else 1.0
    even = [values[i] + values[ORDER - 1 - i] for i in range(half)]
    odd = [values[i] - values[ORDER - 1 - i] for i in range(half)]
    front, back = [], []
    for j in range(half):
        even_sum = odd_sum = None
        for i in range(half):
            ce = float(0.5 * (matrix[j, i] + matrix[j, ORDER - 1 - i]))
            co = float(0.5 * (matrix[j, i] - matrix[j, ORDER - 1 - i]))
            even_sum = even[i] * ce if even_sum is None else even_sum + even[i] * ce
            odd_sum = odd[i] * co if odd_sum is None else odd_sum + odd[i] * co
        front.append(even_sum + odd_sum)
        back.append(flip * (even_sum - odd_sum))
    return front + back[::-1]


def kernel(ndom, nsub, local_barrier, level_ref, velocity_ref, source_ref, planes_ref, wide_ref,
           new_ref, pressure_ref, correction_ref, *scratch):
    (level_v, velocity_v, source_v, planes_v, wide_v, in_sem,
     face_send, face_recv, edge_send, edge_recv, sum_send, sum_recv,
     faces, edges, faces_in, edges_in, sums, sums_in) = scratch
    dom, sub = lax.axis_index("dom"), lax.axis_index("sub")

    def peer(a, b):
        return (lax.rem(dom + a % ndom, ndom), lax.rem(sub + b % nsub, nsub))

    loads = [
        pltpu.make_async_copy(src, dst, in_sem.at[i])
        for i, (src, dst) in enumerate((
            (level_ref, level_v), (planes_ref, planes_v), (wide_ref, wide_v),
            (velocity_ref, velocity_v), (source_ref, source_v)))
    ]
    barrier = pltpu.get_barrier_semaphore()
    near = [(a, b) for a in (-1, 1, 0) for b in (-1, 1, 0) if a or b]
    if local_barrier:
        for a, b in near:
            pl.semaphore_signal(barrier, inc=1, device_id=peer(a, b), device_id_type=MESH)
    else:
        @pl.loop(1, ndom * nsub)
        def _(k):
            target = (lax.rem(dom + k // nsub, ndom), lax.rem(sub + k % nsub, nsub))
            pl.semaphore_signal(barrier, inc=1, device_id=target, device_id_type=MESH)
    for load in loads:
        load.start()

    shape = level_v.shape[1:]
    lane = lax.broadcasted_iota(jnp.int32, shape, 1) % ORDER
    row = lax.broadcasted_iota(jnp.int32, shape, 0)
    lane_first, lane_last = lane == 0, lane == ORDER - 1
    row_first, row_last = row == 0, row == ORDER - 1
    lanes = shape[1]
    span = range(ORDER)

    def fold_lanes(v):
        lower = pltpu.roll(v, 1, 1)
        upper = pltpu.roll(v, lanes - 1, 1)
        return v + jnp.where(lane_last, upper, jnp.where(lane_first, lower, 0.0))

    def along_second(values, kind):
        result = []
        for v in values:
            total = v * planes_v[kind * ORDER]
            for shift in range(1, ORDER):
                total = total + pltpu.roll(v, shift, 0) * planes_v[kind * ORDER + shift]
            result.append(total)
        return result

    def along_third(values, kind):
        stacked = jnp.concatenate(values, axis=0)
        high = stacked.astype(jnp.bfloat16)
        low = (stacked - high.astype(jnp.float32)).astype(jnp.bfloat16)
        out = jnp.dot(jnp.concatenate([high, low], axis=0), wide_v[kind],
                      preferred_element_type=jnp.float32)
        n = ORDER * ORDER
        total = out[:n, :lanes] + (out[:n, lanes:] + out[n:, :lanes])
        return [total[i * ORDER:(i + 1) * ORDER] for i in span]

    def gradient(values):
        third = along_third(values, GRAD)
        return along_first(values, GRAD), along_second(values, GRAD), third

    def divergence(parts, kind):
        third = along_third(parts[2], kind)
        first, second = along_first(parts[0], kind), along_second(parts[1], kind)
        return [(first[i] + second[i]) + third[i] for i in span]

    upper = dom // (ndom // 2)
    ways = ((1 - upper, lax.rem(dom + 2 * upper - 1 + ndom, ndom)),
            (upper, lax.rem(dom - 2 * upper + 1 + ndom, ndom)))

    def begin(step, field):
        face_out, edge_out = faces.at[step], edges.at[step]
        last, first = fold_lanes(field[ORDER - 1]), fold_lanes(field[0])
        face_out[0], face_out[1] = last, first
        edge_out[0], edge_out[1] = last[ORDER - 1:], last[:1]
        edge_out[2], edge_out[3] = first[ORDER - 1:], first[:1]

        def post(out, into, slot, sends, receives, target):
            pltpu.make_async_remote_copy(
                out.at[slot], into.at[step, slot], sends.at[step], receives.at[step],
                device_id=target, device_id_type=MESH).start()

        for slot, beside in ways:
            for j, b in enumerate((1, -1)):
                post(edge_out, edges_in, 2 * slot + j, edge_send, edge_recv,
                     (beside, lax.rem(sub + b % nsub, nsub)))
            post(face_out, faces_in, slot, face_send, face_recv, (beside, sub))
        face_out[2] = fold_lanes(jnp.concatenate([v[ORDER - 1:] for v in field], axis=0))
        face_out[3] = fold_lanes(jnp.concatenate([v[:1] for v in field], axis=0))
        post(face_out, faces_in, 2, face_send, face_recv, peer(0, 1))
        post(face_out, faces_in, 3, face_send, face_recv, peer(0, -1))
        return [first] + [fold_lanes(v) for v in field[1:-1]] + [last]

    def finish(step, field):
        face_in, edge_in = faces_in.at[step], edges_in.at[step]
        pltpu.make_async_copy(face_in, face_in, face_recv.at[step]).wait()
        pltpu.make_async_copy(edge_in, edge_in, edge_recv.at[step]).wait()
        result = list(field)
        for i, at in enumerate((0, ORDER - 1)):
            result[at] = result[at] + face_in[i] + jnp.where(
                row_first, edge_in[2 * i], jnp.where(row_last, edge_in[2 * i + 1], 0.0))
        for i in span:
            result[i] = result[i] + jnp.where(
                row_first, face_in[2, i:i + 1], jnp.where(row_last, face_in[3, i:i + 1], 0.0))
        return result

    def assemble(step, field):
        return finish(step, begin(step, field))

    hops = sorted(range(ndom), key=lambda a: min(a, ndom - a) or ndom)
    others = [(a, b) for a in hops for b in (2, 1, 3, 0) if a or b] if nsub == 4 else [
        (a, b) for a in hops for b in range(nsub) if a or b]

    def begin_sums(step, first, second):
        sums[step, 0:1] = jnp.sum(first, axis=0, keepdims=True)
        sums[step, 1:2] = jnp.sum(second, axis=0, keepdims=True)

        post_sums(step, True)

    def post_sums(step, far):
        def post(target, k):
            pltpu.make_async_remote_copy(
                sums.at[step], sums_in.at[step, k], sum_send.at[step], sum_recv.at[step],
                device_id=target, device_id_type=MESH).start()
        if ndom * nsub <= 64:
            for k, (a, b) in enumerate(others):
                if (k < len(others) // 2) == far:
                    post(peer(a, b), k)
        elif far:
            @pl.loop(1, ndom * nsub)
            def _(k):
                post((lax.rem(dom + k // nsub, ndom), lax.rem(sub + k % nsub, nsub)), k - 1)

    def finish_sums(step):
        pltpu.make_async_copy(sums_in.at[step], sums_in.at[step], sum_recv.at[step]).wait()
        total = sums[step] + jnp.sum(sums_in[step], axis=0)
        total = jnp.sum(total, axis=1, keepdims=True)
        return total[0:1], total[1:2]

    def dot(a, b, scale=None):
        total = None
        for i in span:
            term = a[i] * b[i]
            if scale is not None:
                term = term * scale[i]
            total = term if total is None else total + term
        return total

    for load in loads[:3]:
        load.wait()
    weight_plane = planes_v[3 * ORDER]
    count_plane = planes_v[3 * ORDER + 1]
    weight = [weight_plane * float(WEIGHTS[i]) for i in span]
    inv_mult = [count_plane * float(COUNT[i]) for i in span]

    phi = [level_v[i] for i in span]
    g0, g1, g2 = gradient(phi)
    loads[3].wait()
    advected = [
        phi[i] - advect_step * (velocity_v[0, i] * g0[i] + velocity_v[1, i] * g1[i]
                                + velocity_v[2, i] * g2[i]) for i in span]
    pl.semaphore_wait(barrier, len(near) if local_barrier else ndom * nsub - 1)
    sent = begin(0, advected)
    loads[4].wait()
    sent_right = begin(1, [weight[i] * source_v[i] for i in span])
    phi = finish(0, sent)
    phi = [phi[i] * inv_mult[i] for i in span]

    step = 2
    for sweep in range(SWEEPS):
        g0, g1, g2 = gradient(phi)
        if sweep == 0:
            scaled = [lax.rsqrt(jnp.maximum(
                g0[i] * g0[i] + g1[i] * g1[i] + g2[i] * g2[i], 1.0)) for i in span]
            normals = [[g[i] * scaled[i] for i in span] for g in (g0, g1, g2)]
        compress = [p * (1.0 - p) for p in phi]
        flux = [[interface_width * g[i] - compress[i] * normal[i] for i in span]
                for g, normal in zip((g0, g1, g2), normals)]
        change = assemble(step, divergence(flux, GRAD))
        step += 1
        phi = [phi[i] + reinit_step * change[i] * inv_mult[i] for i in span]

    for i in span:
        new_ref[i] = phi[i]
    weighted = [weight[i] * (1.0 / (1.0 + density_ratio * phi[i] * phi[i])) for i in span]
    squares = divergence([weighted] * 3, SQUARE)
    diagonal = assemble(step, [weight[i] + squares[i] for i in span])
    step += 1
    inverse = [1.0 / v for v in diagonal]

    def apply(step, sum_step, residual, precond):
        slopes = gradient(precond)
        parts = [[weighted[i] * g[i] for i in span] for g in slopes]
        mass = [weight[i] * precond[i] for i in span]
        energy = dot(precond, mass)
        for slope, part in zip(slopes, parts):
            energy = energy + dot(slope, part)
        begin_sums(sum_step, dot(residual, precond, inv_mult), energy)
        total = divergence(parts, TRANS)
        sent = begin(step, [mass[i] + total[i] for i in span])
        post_sums(sum_step, False)
        applied = finish(step, sent)
        return (applied,) + finish_sums(sum_step)

    residual = finish(1, sent_right)
    precond = [residual[i] * inverse[i] for i in span]
    applied, norm_now, product = apply(step, 0, residual, precond)
    step += 1
    step_size = norm_now / product
    direction, image = precond, applied
    result = None
    for it in range(PITERS):
        moved = [step_size * d for d in direction]
        result = moved if result is None else [result[i] + moved[i] for i in span]
        residual = [residual[i] - step_size * image[i] for i in span]
        if it + 1 < PITERS:
            precond = [residual[i] * inverse[i] for i in span]
            applied, norm_next, product = apply(step, it + 1, residual, precond)
            step += 1
            ratio = norm_next / norm_now
            step_size = norm_next / (product - ratio * norm_next / step_size)
            direction = [precond[i] + ratio * direction[i] for i in span]
            image = [applied[i] + ratio * image[i] for i in span]
            norm_now = norm_next
    for i in span:
        pressure_ref[i] = result[i]
        correction_ref[i] = residual[i] * inverse[i]
    for s in range(step):
        pltpu.make_async_copy(faces.at[s], faces.at[s], face_send.at[s]).wait()
        pltpu.make_async_copy(edges.at[s], edges.at[s], edge_send.at[s]).wait()
    for s in range(PITERS):
        pltpu.make_async_copy(sums_in.at[s], sums_in.at[s], sum_send.at[s]).wait()


def write_out(a_in, b_in, c_in, a_out, b_out, c_out, sem):
    copies = [pltpu.make_async_copy(src, dst, sem.at[i]) for i, (src, dst) in enumerate((
        (a_in, a_out), (b_in, b_out), (c_in, c_out)))]
    for copy in copies:
        copy.start()
    for copy in copies:
        copy.wait()


def solution(mesh):
    ndom, nsub = mesh.shape["dom"], mesh.shape["sub"]
    rounds = SWEEPS + 3 + PITERS
    local_barrier = max(ndom, nsub) // 2 <= SWEEPS + 3

    def local(level_set, velocity, source):
        assert level_set.shape[:2] == (ORDER, ORDER)
        lanes = level_set.shape[2]
        planes, wide = constants(lanes)
        tile = (ORDER, lanes)
        vmem = functools.partial(pltpu.VMEM, dtype=jnp.float32)
        others = ndom * nsub - 1
        dma = pltpu.SemaphoreType.DMA
        scratch = [
            vmem(level_set.shape), vmem(velocity.shape), vmem(source.shape),
            vmem(planes.shape), pltpu.VMEM(wide.shape, jnp.bfloat16),
            dma((5,)),
            dma((rounds,)), dma((rounds,)), dma((rounds,)), dma((rounds,)),
            dma((PITERS,)), dma((PITERS,)),
            vmem((rounds, 4) + tile), vmem((rounds, 4, 1, lanes)),
            vmem((rounds, 4) + tile), vmem((rounds, 4, 1, lanes)),
            vmem((PITERS, 2, lanes)), vmem((PITERS, others, 2, lanes)),
        ]
        any_space = pl.BlockSpec(memory_space=pl.ANY)
        hbm_space = pl.BlockSpec(memory_space=pltpu.HBM)
        out = jax.ShapeDtypeStruct(level_set.shape, jnp.float32)
        held = pltpu.VMEM(level_set.shape, jnp.float32)
        results = pl.pallas_call(
            functools.partial(kernel, ndom, nsub, local_barrier),
            out_shape=(held, held, held),
            in_specs=[hbm_space] * 5,
            out_specs=(pl.BlockSpec(memory_space=pltpu.VMEM),) * 3,
            scratch_shapes=scratch,
            compiler_params=pltpu.CompilerParams(
                collective_id=0, has_side_effects=True, vmem_limit_bytes=60 * 2**20),
        )(level_set, velocity, source, jnp.asarray(planes), jnp.asarray(wide))
        return pl.pallas_call(
            write_out,
            out_shape=(out, out, out),
            in_specs=[any_space] * 3,
            out_specs=(hbm_space,) * 3,
            scratch_shapes=[dma((3,))],
            compiler_params=pltpu.CompilerParams(vmem_limit_bytes=2**20),
        )(*results)

    return jax.shard_map(
        local,
        mesh=mesh,
        in_specs=(P("dom", "sub", None), P(None, "dom", "sub", None), P("dom", "sub", None)),
        out_specs=(P("dom", "sub", None), P("dom", "sub", None), P("dom", "sub", None)),
        check_vma=False,
    )
```
